32 devices in a mesh: inp: 8 (over z, y), tm: 4 (over x, core).
Axes of the slice: x: 2, y: 2, z: 4, core: 2. Of those that a mesh axis runs over, the one named last changes fastest.
Arguments:
- voltages: bfloat16 [1024, 262144], P('inp', 'tm'), may hold values from -6 to 6
- pfb_coeff: float32 [16, 512], replicated, may hold values from -1.5 to 1.5
Outputs:
- visibilities: float32 [32, 2, 1024, 1024], P(('inp', 'tm'))
The draws below stay inside these ranges and needn't reach their ends.
All inputs are finite; a program needn't handle non-finite values.
Results may differ from the reference program's by a relative error of at most 0.0029.
Values may be sent and summed in bfloat16 or wider, within the bound.
A program may use at most 128 MiB of HBM per device.

```python
import math
import jax
import jax.numpy as jnp
from jax import lax

INPUTS = 1024
FFT_LEN = 512
TAPS = 16
CHAN = 32
SPECTRA = 512


def shard_levels(stream_key, extent, shards, low, high):
    def one(position, blocks):
        heights = jax.random.uniform(jax.random.fold_in(jax.random.fold_in(stream_key, 6), position), (blocks,), jnp.float32, low / len(shards), high / len(shards))
        return jnp.repeat(jnp.exp(heights), extent[position] // blocks).reshape((-1,) + (1,) * (len(extent) - position - 1))

    level = one(*shards[0])
    for cut in shards[1:]:
        level = level * one(*cut)
    return level


def bell_draw(key, dims, deviation, limit, shards=(), kind=jnp.bfloat16):
    result = jax.random.normal(key, dims, jnp.float32) * deviation
    if len(shards) > 0:
        result = shard_levels(key, dims, shards, -0.22, 0.18) * result
    return jnp.clip(result, min=-limit, max=limit).astype(kind)


def setup_inputs(seed: int = 0) -> dict:
    keys = jax.random.split(jax.random.key(seed), 3)
    voltages = bell_draw(keys[0], (INPUTS, SPECTRA * FFT_LEN), 1.0, 6.0, ((0, 8), (1, 4)))
    pfb_coeff = bell_draw(keys[1], (TAPS, FFT_LEN), TAPS ** -0.5, 1.5, (), jnp.float32)
    return dict(voltages=voltages, pfb_coeff=pfb_coeff)


def reference(voltages, pfb_coeff):
    input_block = math.gcd(INPUTS, 32)
    blocks = voltages.reshape(INPUTS // input_block, input_block, SPECTRA, FFT_LEN)

    def channelize(input_group):
        padded = jnp.concatenate([jnp.zeros((input_block, TAPS - 1, FFT_LEN), input_group.dtype), input_group], axis=1)
        filtered = jnp.zeros((input_block, SPECTRA, FFT_LEN), jnp.float32)
        for tap_index in range(TAPS):
            filtered = filtered + pfb_coeff[tap_index][None, None, :] * padded[:, tap_index:tap_index + SPECTRA, :].astype(jnp.float32)
        spectrum = jnp.fft.rfft(filtered, axis=-1)[:, :, :CHAN]
        norm_scale = 1.0 / math.sqrt(FFT_LEN)
        real_part = (jnp.real(spectrum) * norm_scale).astype(jnp.bfloat16)
        imag_part = (jnp.imag(spectrum) * norm_scale).astype(jnp.bfloat16)
        return jnp.stack([real_part, imag_part], axis=0)
    channelized = lax.map(channelize, blocks)
    channelized = jnp.transpose(channelized, (4, 1, 0, 2, 3)).reshape(CHAN, 2, INPUTS, SPECTRA)

    def gram_matrix(chan_data):
        real_part = chan_data[0].astype(jnp.float32)
        imag_part = chan_data[1].astype(jnp.float32)
        same_pol = jnp.dot(real_part, real_part.T, precision=lax.Precision.HIGHEST, preferred_element_type=jnp.float32)
        same_pol = same_pol + jnp.dot(imag_part, imag_part.T, precision=lax.Precision.HIGHEST, preferred_element_type=jnp.float32)
        cross_term = jnp.dot(imag_part, real_part.T, precision=lax.Precision.HIGHEST, preferred_element_type=jnp.float32)
        return jnp.stack([same_pol, cross_term - cross_term.T], axis=0) * (1.0 / SPECTRA)
    return lax.map(gram_matrix, channelized)
```

```python
import functools
import math

import jax
import jax.numpy as jnp
import numpy as np
from jax import lax
from jax.experimental import pallas as pl
from jax.experimental.pallas import tpu as pltpu
from jax.sharding import PartitionSpec as P

LANES = 128
ROWS = 16
GROUP = 8
CHUNK = 16
NT = (((1,), (1,)), ((), ()))


def dft_tables(channels, length):
    phase = np.arange(channels)[:, None] * np.arange(length)[None, :] % length
    angle = phase * (2.0 * math.pi / length)
    table = np.stack([np.cos(angle), -np.sin(angle)], axis=1) / math.sqrt(length)
    table = table.reshape(2 * channels, length).astype(np.float32)
    high = table.astype(jnp.bfloat16)
    low = (table - high.astype(np.float32)).astype(jnp.bfloat16)
    return np.concatenate([high, low], axis=0)


def channelize_kernel(
    n_inp, n_tm, volt, coef_in, table, out,
    slab, coef, f_high, f_low, stage, send,
    load_sem, tail_send, tail_recv, send_sem, recv_sem,
):
    in_rows = volt.shape[0]
    taps, length = coef_in.shape
    spec = volt.shape[1] // length
    lines = stage.shape[0] // CHUNK
    n_dev = n_inp * n_tm
    chunks = spec // CHUNK
    tail = (taps - 1) * length
    width = CHUNK * length
    a_tiles = in_rows // ROWS
    inp = lax.axis_index("inp")
    tm = lax.axis_index("tm")
    me = inp * n_tm + tm

    def load(q):
        return pltpu.make_async_copy(
            volt.at[:, pl.ds(pl.multiple_of(q * width, width), width)],
            slab.at[:, pl.ds(pl.multiple_of(tail + q * width, length), width)],
            load_sem.at[q],
        )

    for q in range(chunks):
        load(q).start()

    barrier = pltpu.get_barrier_semaphore()

    def greet(d, _):
        other = lax.rem(me + d, n_dev)
        pl.semaphore_signal(
            barrier, inc=1, device_id=(other // n_tm, lax.rem(other, n_tm)),
            device_id_type=pl.DeviceIdType.MESH,
        )
        return _

    lax.fori_loop(1, n_dev, greet, 0)
    for j in range(taps):
        coef[j] = jnp.broadcast_to(coef_in[j : j + 1, :], (8, length))
    pl.semaphore_wait(barrier, n_dev - 1)

    history = pltpu.make_async_remote_copy(
        src_ref=volt.at[:, pl.ds(spec * length - tail, tail)],
        dst_ref=slab.at[:, pl.ds(0, tail)],
        send_sem=tail_send, recv_sem=tail_recv,
        device_id=(inp, lax.rem(tm + 1, n_tm)),
        device_id_type=pl.DeviceIdType.MESH,
    )

    @pl.when(tm < n_tm - 1)
    def _():
        history.start()

    @pl.when(tm == 0)
    def _():
        def clear(e, _):
            slab[:, pl.ds(pl.multiple_of(e * length, length), length)] = jnp.zeros(
                (in_rows, length), slab.dtype
            )
            return _

        lax.fori_loop(0, taps - 1, clear, 0)

    def fir(first, tile, slot):
        row = pl.multiple_of(tile * ROWS, ROWS)
        for nt in range(length // LANES):
            lanes = pl.ds(nt * LANES, LANES)
            c = [coef[j, :, lanes] for j in range(taps)]
            low = [None] * GROUP
            high = [None] * GROUP
            for t in range(GROUP + taps - 1):
                col = pl.multiple_of((first + t) * length + nt * LANES, LANES)
                x = slab[pl.ds(row, ROWS), pl.ds(col, LANES)].astype(jnp.float32)
                x0, x1 = x[:8], x[8:]
                for i in range(max(0, t - taps + 1), min(GROUP - 1, t) + 1):
                    w = c[t - i]
                    if t == i:
                        low[i], high[i] = w * x0, w * x1
                    else:
                        low[i], high[i] = low[i] + w * x0, high[i] + w * x1
                i = t - taps + 1
                if i >= 0:
                    f = jnp.concatenate([low[i], high[i]], axis=0)
                    h = f.astype(jnp.bfloat16)
                    f_high[slot, i, pl.ds(row, ROWS), lanes] = h
                    f_low[slot, i, pl.ds(row, ROWS), lanes] = (
                        f - h.astype(jnp.float32)
                    ).astype(jnp.bfloat16)

    def dft(tile, slot):
        per = GROUP // a_tiles
        for u in range(per):
            i = tile * per + u
            r = lax.dot_general(table[...], f_high[slot, i], NT, preferred_element_type=jnp.float32)
            r2 = lax.dot_general(table[:lines], f_low[slot, i], NT, preferred_element_type=jnp.float32)
            stage[pl.ds(slot * GROUP + i, lines, stride=CHUNK), :] = r[:lines] + r[lines:] + r2

    def each(body):
        def step(tile, _):
            body(tile)
            return _

        lax.fori_loop(0, a_tiles, step, 0)

    def own(q):
        return pltpu.make_async_copy(send.at[q, me], place(out, q), recv_sem)

    def place(ref, q):
        first = pl.multiple_of(tm * spec + q * CHUNK, CHUNK)
        return ref.at[inp, :, pl.ds(first, CHUNK), :]

    def dispatch(q):
        def convert(d, _):
            rows = pl.ds(pl.multiple_of(d * 2 * CHUNK, 2 * CHUNK), 2 * CHUNK)
            send[q, d] = stage[rows, :].reshape(2, CHUNK, in_rows).astype(send.dtype)
            return _

        lax.fori_loop(0, n_dev, convert, 0)

        def post(d, _):
            other = lax.rem(me + d, n_dev)
            pltpu.make_async_remote_copy(
                src_ref=send.at[q, other], dst_ref=place(out, q),
                send_sem=send_sem, recv_sem=recv_sem,
                device_id=(other // n_tm, lax.rem(other, n_tm)),
                device_id_type=pl.DeviceIdType.MESH,
            ).start()
            return _

        lax.fori_loop(1, n_dev, post, 0)
        own(q).start()

    def chunk_of(k):
        return lax.rem(k + 1, chunks)

    load(0).wait()
    load(1).wait()
    each(lambda tile: fir(chunk_of(0) * CHUNK, tile, 0))

    def turn(k, carry):
        q = chunk_of(k)
        later = chunk_of(k + 1)

        def second(tile):
            fir(q * CHUNK + GROUP, tile, 1)
            dft(tile, 0)

        each(second)

        @pl.when(later > 0)
        def _():
            load(later).wait()

        @pl.when((later == 0) & (tm > 0))
        def _():
            history.wait_recv()

        def first(tile):
            fir(later * CHUNK, tile, 0)
            dft(tile, 1)

        each(first)
        dispatch(q)
        return carry

    lax.fori_loop(0, chunks - 1, turn, 0)

    def final(tile):
        fir(GROUP, tile, 1)
        dft(tile, 0)

    each(final)
    each(lambda tile: dft(tile, 1))
    dispatch(0)

    @pl.when(tm < n_tm - 1)
    def _():
        history.wait_send()

    sent = send.at[:, pl.ds(0, n_dev - 1)]
    pltpu.make_async_copy(sent, sent, send_sem).wait()
    pltpu.make_async_copy(out, out, recv_sem).wait()


def correlate_kernel(z_ref, o_ref, wide, turned, crossed):
    groups, _, spectra, in_rows = z_ref.shape
    block = o_ref.shape[2]

    @pl.when(pl.program_id(0) == 0)
    def _():
        for g in range(groups):
            cols = slice(g * in_rows, (g + 1) * in_rows)
            for p in range(2):
                part = z_ref[g, p]
                wide[p * spectra : (p + 1) * spectra, cols] = part
                flip = part.T
                turned[cols, p * spectra : (p + 1) * spectra] = flip
                crossed[cols, (1 - p) * spectra : (2 - p) * spectra] = flip if p else -flip

    rows = pl.ds(pl.multiple_of(pl.program_id(0) * block, block), block)
    scale = 1.0 / spectra
    o_ref[0, 0] = jnp.dot(turned[rows, :], wide[...], preferred_element_type=jnp.float32) * scale
    o_ref[0, 1] = jnp.dot(crossed[rows, :], wide[...], preferred_element_type=jnp.float32) * scale


def per_device(voltages, pfb_coeff):
    n_inp = lax.axis_size("inp")
    n_tm = lax.axis_size("tm")
    channels = n_inp * n_tm
    in_rows = voltages.shape[0]
    taps, length = pfb_coeff.shape
    spec = voltages.shape[1] // length
    lines = 2 * channels
    table = jnp.asarray(dft_tables(channels, length))
    vmem = pl.BlockSpec(memory_space=pltpu.VMEM)
    hbm = pl.BlockSpec(memory_space=pl.ANY)
    bf16 = jnp.bfloat16
    received = pl.pallas_call(
        functools.partial(channelize_kernel, n_inp, n_tm),
        out_shape=jax.ShapeDtypeStruct((n_inp, 2, n_tm * spec, in_rows), bf16),
        in_specs=[hbm, vmem, vmem],
        out_specs=hbm,
        scratch_shapes=[
            pltpu.VMEM((in_rows, (spec + taps - 1) * length), bf16),
            pltpu.VMEM((taps, 8, length), jnp.float32),
            pltpu.VMEM((2, GROUP, in_rows, length), bf16),
            pltpu.VMEM((2, GROUP, in_rows, length), bf16),
            pltpu.VMEM((lines * CHUNK, in_rows), jnp.float32),
            pltpu.VMEM((spec // CHUNK, channels, 2, CHUNK, in_rows), bf16),
            pltpu.SemaphoreType.DMA((spec // CHUNK,)),
            pltpu.SemaphoreType.DMA,
            pltpu.SemaphoreType.DMA,
            pltpu.SemaphoreType.DMA,
            pltpu.SemaphoreType.DMA,
        ],
        compiler_params=pltpu.CompilerParams(
            collective_id=0, has_side_effects=True, vmem_limit_bytes=60 * 1024 * 1024
        ),
        name="channelize",
    )(voltages, pfb_coeff, table)
    inputs = n_inp * in_rows
    spectra = n_tm * spec
    block = min(256, inputs)
    return pl.pallas_call(
        correlate_kernel,
        grid=(inputs // block,),
        out_shape=jax.ShapeDtypeStruct((1, 2, inputs, inputs), jnp.float32),
        in_specs=[pl.BlockSpec(received.shape, lambda i: (0, 0, 0, 0))],
        out_specs=pl.BlockSpec((1, 2, block, inputs), lambda i: (0, 0, i, 0)),
        scratch_shapes=[
            pltpu.VMEM((2 * spectra, inputs), bf16),
            pltpu.VMEM((inputs, 2 * spectra), bf16),
            pltpu.VMEM((inputs, 2 * spectra), bf16),
        ],
        compiler_params=pltpu.CompilerParams(vmem_limit_bytes=60 * 1024 * 1024),
        name="correlate",
    )(received)


def solution(mesh):
    return jax.shard_map(
        per_device,
        mesh=mesh,
        in_specs=(P("inp", "tm"), P()),
        out_specs=P(("inp", "tm"), None, None, None),
        check_vma=False,
    )
```

```python
import functools
import math

import jax
import jax.numpy as jnp
import numpy as np
from jax import lax
from jax.experimental import pallas as pl
from jax.experimental.pallas import tpu as pltpu
from jax.sharding import PartitionSpec as P

LANES = 128
ROWS = 16
GROUP = 8
CHUNK = 16
NT = (((1,), (1,)), ((), ()))


def dft_tables(channels, length):
    phase = np.arange(channels)[:, None] * np.arange(length)[None, :] % length
    angle = phase * (2.0 * math.pi / length)
    table = np.stack([np.cos(angle), -np.sin(angle)], axis=1) / math.sqrt(length)
    table = table.reshape(2 * channels, length).astype(np.float32)
    high = table.astype(jnp.bfloat16)
    low = (table - high.astype(np.float32)).astype(jnp.bfloat16)
    return np.concatenate([high, low], axis=0)


def channelize_kernel(
    n_inp, n_tm, volt, coef_in, table, out,
    slab, coef, high0, low0, high1, low1, stage, send,
    load_sem, tail_send, tail_recv, send_sem, recv_sem,
):
    in_rows = volt.shape[0]
    taps, length = coef_in.shape
    spec = volt.shape[1] // length
    lines = stage.shape[0] // CHUNK
    n_dev = n_inp * n_tm
    chunks = spec // CHUNK
    tail = (taps - 1) * length
    width = CHUNK * length
    a_tiles = in_rows // ROWS
    inp = lax.axis_index("inp")
    tm = lax.axis_index("tm")
    me = inp * n_tm + tm

    def load(q):
        return pltpu.make_async_copy(
            volt.at[:, pl.ds(pl.multiple_of(q * width, width), width)],
            slab.at[:, pl.ds(pl.multiple_of(tail + q * width, length), width)],
            load_sem.at[q],
        )

    load(0).start()
    load(1).start()

    barrier = pltpu.get_barrier_semaphore()

    def greet(d, _):
        other = lax.rem(me + d, n_dev)
        pl.semaphore_signal(
            barrier, inc=1, device_id=(other // n_tm, lax.rem(other, n_tm)),
            device_id_type=pl.DeviceIdType.MESH,
        )
        return _

    lax.fori_loop(1, n_dev, greet, 0)
    for j in range(taps):
        coef[j] = jnp.broadcast_to(coef_in[j : j + 1, :], (8, length))
    @pl.when(tm == 0)
    def _():
        def clear(e, _):
            slab[:, pl.ds(pl.multiple_of(e * length, length), length)] = jnp.zeros(
                (in_rows, length), slab.dtype
            )
            return _

        lax.fori_loop(0, taps - 1, clear, 0)

    f_high, f_low = (high0, high1), (low0, low1)

    def fir(first, tile, slot):
        row = pl.multiple_of(tile * ROWS, ROWS)
        for nt in range(length // LANES):
            lanes = pl.ds(nt * LANES, LANES)
            c = [coef[j, :, lanes] for j in range(taps)]
            low = [None] * GROUP
            high = [None] * GROUP
            for t in range(GROUP + taps - 1):
                col = pl.multiple_of((first + t) * length + nt * LANES, LANES)
                x = slab[pl.ds(row, ROWS), pl.ds(col, LANES)].astype(jnp.float32)
                x0, x1 = x[:8], x[8:]
                for i in range(max(0, t - taps + 1), min(GROUP - 1, t) + 1):
                    w = c[t - i]
                    if t == i:
                        low[i], high[i] = w * x0, w * x1
                    else:
                        low[i], high[i] = low[i] + w * x0, high[i] + w * x1
                i = t - taps + 1
                if i >= 0:
                    f = jnp.concatenate([low[i], high[i]], axis=0)
                    h = f.astype(jnp.bfloat16)
                    f_high[slot][i, pl.ds(row, ROWS), lanes] = h
                    f_low[slot][i, pl.ds(row, ROWS), lanes] = (
                        f - h.astype(jnp.float32)
                    ).astype(jnp.bfloat16)

    def dft(tile, slot):
        per = GROUP // a_tiles
        for u in range(per):
            i = tile * per + u
            r = lax.dot_general(table[...], f_high[slot][i], NT, preferred_element_type=jnp.float32)
            r2 = lax.dot_general(table[:lines], f_low[slot][i], NT, preferred_element_type=jnp.float32)
            stage[pl.ds(slot * GROUP + i, lines, stride=CHUNK), :] = r[:lines] + r[lines:] + r2

    def each(body):
        def step(tile, _):
            body(tile)
            return _

        lax.fori_loop(0, a_tiles, step, 0)

    def own(q):
        return pltpu.make_async_copy(send.at[q, me], place(out, q), recv_sem)

    def place(ref, q):
        first = pl.multiple_of(tm * spec + q * CHUNK, CHUNK)
        return ref.at[inp, :, pl.ds(first, CHUNK), :]

    def dispatch(q):
        def convert(d, _):
            rows = pl.ds(pl.multiple_of(d * 2 * CHUNK, 2 * CHUNK), 2 * CHUNK)
            send[q, d] = stage[rows, :].reshape(2, CHUNK, in_rows).astype(send.dtype)
            return _

        lax.fori_loop(0, n_dev, convert, 0)

        def post(d, _):
            other = lax.rem(me + d, n_dev)
            pltpu.make_async_remote_copy(
                src_ref=send.at[q, other], dst_ref=place(out, q),
                send_sem=send_sem, recv_sem=recv_sem,
                device_id=(other // n_tm, lax.rem(other, n_tm)),
                device_id_type=pl.DeviceIdType.MESH,
            ).start()
            return _

        lax.fori_loop(1, n_dev, post, 0)
        own(q).start()

    def chunk_of(k):
        return lax.rem(k + 1, chunks)

    load(0).wait()
    load(1).wait()
    for q in range(2, chunks):
        load(q).start()
    each(lambda tile: fir(chunk_of(0) * CHUNK, tile, 0))
    pl.semaphore_wait(barrier, n_dev - 1)

    history = pltpu.make_async_remote_copy(
        src_ref=volt.at[:, pl.ds(spec * length - tail, tail)],
        dst_ref=slab.at[:, pl.ds(0, tail)],
        send_sem=tail_send, recv_sem=tail_recv,
        device_id=(inp, lax.rem(tm + 1, n_tm)),
        device_id_type=pl.DeviceIdType.MESH,
    )

    @pl.when(tm < n_tm - 1)
    def _():
        history.start()

    def turn(k, carry):
        q = chunk_of(k)
        later = chunk_of(k + 1)

        def second(tile):
            dft(tile, 0)
            fir(q * CHUNK + GROUP, tile, 1)

        each(second)

        @pl.when(later > 0)
        def _():
            load(later).wait()

        @pl.when((later == 0) & (tm > 0))
        def _():
            history.wait_recv()

        def first(tile):
            dft(tile, 1)
            fir(later * CHUNK, tile, 0)

        each(first)
        dispatch(q)
        return carry

    lax.fori_loop(0, chunks - 1, turn, 0)

    def final(tile):
        dft(tile, 0)
        fir(GROUP, tile, 1)

    each(final)
    each(lambda tile: dft(tile, 1))
    dispatch(0)

    @pl.when(tm < n_tm - 1)
    def _():
        history.wait_send()

    sent = send.at[:, pl.ds(0, n_dev - 1)]
    pltpu.make_async_copy(sent, sent, send_sem).wait()
    pltpu.make_async_copy(out, out, recv_sem).wait()


def correlate_kernel(z_ref, o_ref, wide, turned, crossed):
    groups, _, spectra, in_rows = z_ref.shape
    block = o_ref.shape[2]

    @pl.when(pl.program_id(0) == 0)
    def _():
        for g in range(groups):
            cols = slice(g * in_rows, (g + 1) * in_rows)
            for p in range(2):
                part = z_ref[g, p]
                wide[p * spectra : (p + 1) * spectra, cols] = part
                flip = part.T
                turned[cols, p * spectra : (p + 1) * spectra] = flip
                crossed[cols, (1 - p) * spectra : (2 - p) * spectra] = flip if p else -flip

    rows = pl.ds(pl.multiple_of(pl.program_id(0) * block, block), block)
    scale = 1.0 / spectra
    o_ref[0, 0] = jnp.dot(turned[rows, :], wide[...], preferred_element_type=jnp.float32) * scale
    o_ref[0, 1] = jnp.dot(crossed[rows, :], wide[...], preferred_element_type=jnp.float32) * scale


def per_device(voltages, pfb_coeff):
    n_inp = lax.axis_size("inp")
    n_tm = lax.axis_size("tm")
    channels = n_inp * n_tm
    in_rows = voltages.shape[0]
    taps, length = pfb_coeff.shape
    spec = voltages.shape[1] // length
    lines = 2 * channels
    table = jnp.asarray(dft_tables(channels, length))
    vmem = pl.BlockSpec(memory_space=pltpu.VMEM)
    hbm = pl.BlockSpec(memory_space=pl.ANY)
    bf16 = jnp.bfloat16
    received = pl.pallas_call(
        functools.partial(channelize_kernel, n_inp, n_tm),
        out_shape=jax.ShapeDtypeStruct((n_inp, 2, n_tm * spec, in_rows), bf16),
        in_specs=[hbm, vmem, vmem],
        out_specs=hbm,
        scratch_shapes=[
            pltpu.VMEM((in_rows, (spec + taps - 1) * length), bf16),
            pltpu.VMEM((taps, 8, length), jnp.float32),
            pltpu.VMEM((GROUP, in_rows, length), bf16),
            pltpu.VMEM((GROUP, in_rows, length), bf16),
            pltpu.VMEM((GROUP, in_rows, length), bf16),
            pltpu.VMEM((GROUP, in_rows, length), bf16),
            pltpu.VMEM((lines * CHUNK, in_rows), jnp.float32),
            pltpu.VMEM((spec // CHUNK, channels, 2, CHUNK, in_rows), bf16),
            pltpu.SemaphoreType.DMA((spec // CHUNK,)),
            pltpu.SemaphoreType.DMA,
            pltpu.SemaphoreType.DMA,
            pltpu.SemaphoreType.DMA,
            pltpu.SemaphoreType.DMA,
        ],
        compiler_params=pltpu.CompilerParams(
            collective_id=0, has_side_effects=True, vmem_limit_bytes=60 * 1024 * 1024
        ),
        name="channelize",
    )(voltages, pfb_coeff, table)
    inputs = n_inp * in_rows
    spectra = n_tm * spec
    block = min(256, inputs)
    return pl.pallas_call(
        correlate_kernel,
        grid=(inputs // block,),
        out_shape=jax.ShapeDtypeStruct((1, 2, inputs, inputs), jnp.float32),
        in_specs=[pl.BlockSpec(received.shape, lambda i: (0, 0, 0, 0))],
        out_specs=pl.BlockSpec((1, 2, block, inputs), lambda i: (0, 0, i, 0)),
        scratch_shapes=[
            pltpu.VMEM((2 * spectra, inputs), bf16),
            pltpu.VMEM((inputs, 2 * spectra), bf16),
            pltpu.VMEM((inputs, 2 * spectra), bf16),
        ],
        compiler_params=pltpu.CompilerParams(vmem_limit_bytes=60 * 1024 * 1024),
        name="correlate",
    )(received)


def solution(mesh):
    return jax.shard_map(
        per_device,
        mesh=mesh,
        in_specs=(P("inp", "tm"), P()),
        out_specs=P(("inp", "tm"), None, None, None),
        check_vma=False,
    )
```
